32 devices in a mesh: dp: 4 (over y, z), ep: 8 (over x, core).
Axes of the slice: x: 4, y: 2, z: 2, core: 2. Of those that a mesh axis runs over, the one named last changes fastest.
The devices are a block of a 4x4x8 slice.
Arguments:
- tokens: bfloat16 [4096, 2048], P(('dp', 'ep')), parts along dimension 0
- expert_ids: int32 [4096, 8], P(('dp', 'ep')), parts along dimension 0
- norm_gain: bfloat16 [2048], replicated
- w_router: bfloat16 [2048, 64], replicated
- w_gate: bfloat16 [64, 2048, 1024], P('ep')
- w_up: bfloat16 [64, 2048, 1024], P('ep')
- w_down: bfloat16 [64, 1024, 2048], P('ep')
Outputs:
- output: bfloat16 [4096, 2048], P(('dp', 'ep')), parts along dimension 0
There are 4 independent parts. The reference program is written for one: setup_inputs(seed, part) draws one part's arguments, and reference() takes and returns one part's arrays. A program takes and returns all parts, laid end to end along the dimension named above; an argument that names none is the same for every part.
All inputs are finite; a program needn't handle non-finite values.
Results may differ from the reference program's by a relative error of at most 0.00573975.
Values are sent between devices in bfloat16 or wider.
A program may use at most 768 MiB of HBM per device.

```python
import jax
import jax.numpy as jnp
from jax import lax

D = 2048
EXPERTS = 64
TOP = 8
FF = 1024
TOKENS_DEV = 128
EP_SIZE = 8
BLOCK_ROWS = 128

TOKENS = EP_SIZE * TOKENS_DEV
PAIRS = TOKENS * TOP
E_LOCAL = EXPERTS // EP_SIZE
NUM_BLOCKS = PAIRS // BLOCK_ROWS + EXPERTS + 1
NORM_EPS = 1e-5


def draw_routes(route_key):
    sub_keys = jax.random.split(route_key, 6)
    pair_dev = TOKENS_DEV * TOP
    half_mean = pair_dev // (2 * EP_SIZE)
    hot_dev = jax.random.randint(sub_keys[0], (), 0, EP_SIZE)
    rotation = jax.random.randint(sub_keys[1], (), 0, EP_SIZE - 1)
    rest_weight = jax.random.randint(sub_keys[2], (EP_SIZE - 2,), 1, 3)
    rest_cum = jnp.concatenate([jnp.zeros((1,), jnp.int32), jnp.cumsum(rest_weight)])
    rest_bound = (pair_dev - 7 * half_mean) * rest_cum // rest_cum[-1]
    pattern = jnp.concatenate([jnp.full((1,), 4 * half_mean, jnp.int32), rest_bound[1:] - rest_bound[:-1]])
    src_dev = jnp.arange(EP_SIZE)[:, None]
    dst_dev = jnp.arange(EP_SIZE)[None, :]
    shift_idx = ((dst_dev - hot_dev - 1) % EP_SIZE - src_dev - rotation) % (EP_SIZE - 1)
    dev_load = jnp.where(dst_dev == hot_dev, 3 * half_mean, pattern[shift_idx])
    split_weight = jax.random.randint(sub_keys[3], (EP_SIZE, EP_SIZE, E_LOCAL), 1, 4)
    split_cum = jnp.concatenate([jnp.zeros((EP_SIZE, EP_SIZE, 1), jnp.int32), jnp.cumsum(split_weight, axis=2)], axis=2)
    split_bound = dev_load[:, :, None] * split_cum // split_cum[:, :, -1:]
    expert_count = (split_bound[:, :, 1:] - split_bound[:, :, :-1]).reshape(EP_SIZE, EXPERTS)
    count_end = jnp.cumsum(expert_count, axis=1)
    positions = jnp.arange(pair_dev)
    sorted_ids = jax.vmap(lambda end_row: jnp.searchsorted(end_row, positions, side='right'))(count_end)
    by_token = sorted_ids.reshape(EP_SIZE, TOP, TOKENS_DEV).transpose(0, 2, 1)
    tok_perm = jax.vmap(lambda perm_key: jax.random.permutation(perm_key, TOKENS_DEV))(jax.random.split(sub_keys[4], EP_SIZE))
    by_token = jnp.take_along_axis(by_token, jnp.broadcast_to(tok_perm[:, :, None], (EP_SIZE, TOKENS_DEV, TOP)), axis=1)
    turn = jax.random.randint(sub_keys[5], (EP_SIZE, TOKENS_DEV, 1), 0, TOP)
    col_idx = (jnp.arange(TOP)[None, None, :] + turn) % TOP
    by_token = jnp.take_along_axis(by_token, col_idx, axis=2)
    return by_token.reshape(TOKENS, TOP).astype(jnp.int32)


def setup_inputs(seed: int = 0, part: int = 0) -> dict:
    part_key = jax.random.fold_in(jax.random.key(seed), part)
    tok_key, route_key = jax.random.split(part_key)
    shared = jax.random.split(jax.random.key(seed + 1), 5)
    tokens = jax.random.normal(tok_key, (TOKENS, D), jnp.float32).astype(jnp.bfloat16)
    norm_gain = (1.0 + 0.3 * jax.random.normal(shared[0], (D,), jnp.float32)).astype(jnp.bfloat16)
    w_router = (jax.random.normal(shared[1], (D, EXPERTS), jnp.float32) * D ** -0.5).astype(jnp.bfloat16)
    w_gate = (jax.random.normal(shared[2], (EXPERTS, D, FF), jnp.float32) * D ** -0.5).astype(jnp.bfloat16)
    w_up = (jax.random.normal(shared[3], (EXPERTS, D, FF), jnp.float32) * D ** -0.5).astype(jnp.bfloat16)
    w_down = (jax.random.normal(shared[4], (EXPERTS, FF, D), jnp.float32) * (EXPERTS / 4 * FF ** -0.5)).astype(jnp.bfloat16)
    expert_ids = draw_routes(route_key)
    return {'tokens': tokens, 'expert_ids': expert_ids, 'norm_gain': norm_gain, 'w_router': w_router, 'w_gate': w_gate, 'w_up': w_up, 'w_down': w_down}


def reference(tokens, expert_ids, norm_gain, w_router, w_gate, w_up, w_down):
    tok32 = tokens.astype(jnp.float32)
    inv_rms = lax.rsqrt(jnp.mean(tok32 * tok32, axis=1, keepdims=True) + NORM_EPS)
    normed = (tok32 * inv_rms * norm_gain.astype(jnp.float32)).astype(jnp.bfloat16)
    logits = jnp.dot(normed, w_router, preferred_element_type=jnp.float32)
    router_prob = jax.nn.softmax(logits, axis=1)
    gate_vals = jnp.take_along_axis(router_prob, expert_ids, axis=1)
    flat_ids = expert_ids.reshape(PAIRS)
    sort_order = jnp.argsort(flat_ids, stable=True)
    sorted_ids = flat_ids[sort_order]
    counts = jnp.bincount(flat_ids, length=EXPERTS)
    padded = (counts + BLOCK_ROWS - 1) // BLOCK_ROWS * BLOCK_ROWS
    pad_end = jnp.cumsum(padded)
    group_start = jnp.cumsum(counts) - counts
    slot_sorted = pad_end[sorted_ids] - padded[sorted_ids] + jnp.arange(PAIRS) - group_start[sorted_ids]
    row_buf = jnp.zeros((NUM_BLOCKS * BLOCK_ROWS, D), jnp.bfloat16).at[slot_sorted].set(normed[sort_order // TOP])
    block_expert = jnp.minimum(jnp.searchsorted(pad_end, jnp.arange(NUM_BLOCKS) * BLOCK_ROWS, side='right'), EXPERTS - 1)

    def block_apply(block_args):
        block_rows, expert = block_args
        hidden_gate = jnp.dot(block_rows, w_gate[expert], preferred_element_type=jnp.float32)
        hidden_up = jnp.dot(block_rows, w_up[expert], preferred_element_type=jnp.float32)
        swiglu_out = (jax.nn.silu(hidden_gate) * hidden_up).astype(jnp.bfloat16)
        return jnp.dot(swiglu_out, w_down[expert], preferred_element_type=jnp.float32).astype(jnp.bfloat16)

    block_out = lax.map(block_apply, (row_buf.reshape(NUM_BLOCKS, BLOCK_ROWS, D), block_expert))
    slot_pair = jnp.zeros((PAIRS,), jnp.int32).at[sort_order].set(slot_sorted)
    pair_out = block_out.reshape(NUM_BLOCKS * BLOCK_ROWS, D)[slot_pair].reshape(TOKENS, TOP, D)
    moe_sum = jnp.einsum('nk,nkd->nd', gate_vals, pair_out.astype(jnp.float32))
    return (tok32 + moe_sum).astype(jnp.bfloat16)
```

```python
import functools

import jax
import jax.numpy as jnp
from jax import lax
from jax.experimental import pallas as pl
from jax.experimental.pallas import tpu as pltpu
from jax.sharding import PartitionSpec as P

NORM_EPS = 1e-5
BR = 128
WIN = 256
ALIGN = 16
CW = 256
LAG = 5
F32 = jnp.float32
BF16 = jnp.bfloat16
MESH = pl.DeviceIdType.MESH
ANY = pl.BlockSpec(memory_space=pl.ANY)
VM = pl.BlockSpec(memory_space=pltpu.VMEM)
SM = pl.BlockSpec(memory_space=pltpu.SMEM)


def ring_ids(n_dev):
    me = lax.axis_index('ep')
    n_chip = n_dev // 2
    chip, core = me // 2, me % 2
    right = ((chip + 1) % n_chip) * 2 + core
    left = ((chip + n_chip - 1) % n_chip) * 2 + core
    partner = chip * 2 + (1 - core)
    return me, chip, core, right, left, partner


def enter(peers):
    barrier = pltpu.get_barrier_semaphore()
    for peer in peers:
        pl.semaphore_signal(barrier, inc=1, device_id={'ep': peer}, device_id_type=MESH)
    return lambda: pl.semaphore_wait(barrier, len(peers))


def dispatch_kernel(n_dev, nb, x_ref, g_ref, wr_ref, ids_ref, xs_out, pt_out, gb_out, tab_out,
                    u, p, xs, pt, gb, tab, ids, posm, ids_ssem, ids_rsem, ssem, rsem, osem):
    me, chip, core, right, left, partner = ring_ids(n_dev)
    n_chip = n_dev // 2
    tok = x_ref.shape[0]
    half = tok // 2
    e_local = 8
    opp = (chip + 2) % n_chip
    others = [(me + i) % n_dev for i in range(1, n_dev)]
    wait_entry = enter(others)

    gain = g_ref[...].astype(F32)
    step = tok // 4
    for i in range(4):
        x32 = x_ref[i * step:(i + 1) * step, :].astype(F32)
        inv = lax.rsqrt(jnp.mean(x32 * x32, axis=1, keepdims=True) + NORM_EPS)
        u[me, i * step:(i + 1) * step, :] = (x32 * inv * gain).astype(BF16)
    wait_entry()

    for i, peer in enumerate(others):
        pltpu.make_async_remote_copy(ids_ref, ids.at[me], ids_ssem.at[i], ids_rsem.at[me],
                                     device_id={'ep': peer}, device_id_type=MESH).start()

    def send(i, blk, h, peer):
        ref = u.at[blk, pl.ds(h * half, half), :]
        return pltpu.make_async_remote_copy(ref, ref, ssem.at[i], rsem.at[blk, h],
                                            device_id={'ep': peer}, device_id_type=MESH)

    sends = [send(0, me, 0, right), send(1, me, 1, left), send(2, me, 0, partner), send(3, me, 1, partner),
             send(4, me, 1, right), send(5, me, 0, left)]
    for s in sends:
        s.start()

    def arrived(blk, h):
        send(0, blk, h, partner).wait_recv()

    def forward(i, blk, h, peer):
        s = send(i, blk, h, peer)
        s.start()
        sends.append(s)

    ids[me] = ids_ref[...]
    for i in range(1, n_dev):
        src = (me + i) % n_dev
        pltpu.make_async_remote_copy(ids_ref, ids.at[src], ids_ssem.at[0], ids_rsem.at[src],
                                     device_id={'ep': partner}, device_id_type=MESH).wait_recv()
    sub = lax.broadcasted_iota(jnp.int32, (e_local, tok), 0)
    gid = sub + me * e_local
    hits = []
    for s in range(n_dev):
        hit = jnp.zeros((e_local, tok), jnp.int32)
        for j in range(ids_ref.shape[0]):
            hit = hit + (ids[s, j:j + 1, :] == gid).astype(jnp.int32)
        hits.append(hit.astype(F32))
    hit_all = jnp.concatenate(hits, axis=0).astype(BF16)
    ri = lax.broadcasted_iota(jnp.int32, (tok, tok), 0)
    ci = lax.broadcasted_iota(jnp.int32, (tok, tok), 1)
    before = (ri < ci).astype(F32).astype(BF16)
    cnt_all = jnp.dot(hit_all, jnp.ones((tok, tok), BF16), preferred_element_type=F32)
    rank_all = jnp.dot(hit_all, before, preferred_element_type=F32)
    total = jnp.zeros((e_local, tok), F32)
    for s in range(n_dev):
        total = total + cnt_all[s * e_local:(s + 1) * e_local, :]
    blocks = jnp.floor((total + (BR - 1)) * (1.0 / BR))
    first = jnp.zeros((e_local, tok), F32)
    for e in range(e_local - 1):
        first = first + jnp.where(sub > e, jnp.broadcast_to(blocks[e:e + 1, :], (e_local, tok)), 0.0)
    last = first + blocks
    lane = lax.broadcasted_iota(jnp.int32, (e_local, tok), 1).astype(F32)
    blk_exp = jnp.sum(jnp.where(lane >= last, 1.0, 0.0), axis=0, keepdims=True)
    tab[0:8, :] = blocks.astype(jnp.int32)
    tab[8:16, :] = first.astype(jnp.int32)
    tab[16:24, :] = jnp.broadcast_to(jnp.minimum(blk_exp, e_local - 1.0), (8, tok)).astype(jnp.int32)
    carry = jnp.zeros((e_local, tok), F32)
    wlane = lax.broadcasted_iota(jnp.int32, (tok, WIN), 1).astype(F32)
    for s in range(n_dev):
        run = first * BR + carry
        pos = run + rank_all[s * e_local:(s + 1) * e_local, :]
        start = jnp.floor(run * (1.0 / ALIGN)) * ALIGN
        tab[24 + s * 8:32 + s * 8, :] = (start * (1.0 / ALIGN)).astype(jnp.int32)
        rel = jnp.where(hits[s] > 0, pos - start, -1.0)
        posm[s * 8:(s + 1) * 8, :] = jnp.where(hits[s] > 0, pos + 1.0, 0.0)
        rel_t = jnp.concatenate([rel, jnp.zeros((tok - e_local, tok), F32)], axis=0).T
        par = (s % 2 + core + 1) % 2
        for e in range(e_local):
            col = jnp.broadcast_to(rel_t[:, e:e + 1], (tok, WIN))
            pt[par, s // 2, e] = jnp.where(col == wlane, 1.0, 0.0).astype(BF16)
        carry = carry + cnt_all[s * e_local:(s + 1) * e_local, :]
    row_i = lax.broadcasted_iota(jnp.int32, (BR, tok), 0).astype(F32)

    @pl.loop(0, nb)
    def _(b):
        bf = b.astype(F32)
        mine = (first <= bf) & (bf < last)
        for s in range(n_dev):
            sel = jnp.sum(jnp.where(mine, posm[s * 8:(s + 1) * 8, :], 0.0), axis=0, keepdims=True) - (1.0 + BR * bf)
            p[s // 2, pl.ds(pl.multiple_of(b * BR, BR), BR), (s % 2) * tok:(s % 2 + 1) * tok] = jnp.where(
                jnp.broadcast_to(sel, (BR, tok)) == row_i, 1.0, 0.0).astype(BF16)

    tab_copy = pltpu.make_async_copy(tab, tab_out, osem.at[0])
    tab_copy.start()
    pt_copy = pltpu.make_async_copy(pt, pt_out, osem.at[1])
    pt_copy.start()

    def gates(c):
        for k in range(2):
            blk = c * 2 + k
            logits = jnp.dot(u[blk], wr_ref[...], preferred_element_type=F32)
            ex = jnp.exp(logits - jnp.max(logits, axis=1, keepdims=True))
            prob = ex / jnp.sum(ex, axis=1, keepdims=True)
            par = (k + core + 1) % 2
            for e in range(e_local):
                gb[par, c, e] = jnp.broadcast_to(prob[:, e:e + 1], (tok, 128))

    width = u.shape[2]
    nt = 512

    def gather(c, first_pass):
        @pl.loop(0, nb)
        def _(b):
            rows = pl.ds(pl.multiple_of(b * BR, BR), BR)
            pb = p[c, rows, :]
            for n in range(width // nt):
                uc = jnp.concatenate([u[c * 2, :, n * nt:(n + 1) * nt], u[c * 2 + 1, :, n * nt:(n + 1) * nt]], axis=0)
                part = jnp.dot(pb, uc, preferred_element_type=F32).astype(BF16)
                if first_pass:
                    xs[rows, n * nt:(n + 1) * nt] = part
                else:
                    xs[rows, n * nt:(n + 1) * nt] = xs[rows, n * nt:(n + 1) * nt] + part

    arrived(left, 0)
    forward(6, left, 0, right)
    arrived(right, 1)
    forward(7, right, 1, left)
    forward(8, left, 0, partner)
    forward(9, right, 1, partner)
    arrived(partner, 0)
    arrived(partner, 1)
    gates(chip)
    gather(chip, True)
    arrived(left, 1)
    forward(10, left, 1, partner)
    arrived(right, 0)
    forward(11, right, 0, partner)
    lchip, rchip = (chip + n_chip - 1) % n_chip, (chip + 1) % n_chip
    for blk in (lchip * 2 + (1 - core), rchip * 2 + (1 - core)):
        arrived(blk, 0)
        arrived(blk, 1)
    gates(lchip)
    gather(lchip, False)
    oblk = opp * 2 + core
    arrived(oblk, 0)
    forward(12, oblk, 0, partner)
    arrived(oblk, 1)
    forward(13, oblk, 1, partner)
    gates(rchip)
    gather(rchip, False)
    arrived(opp * 2 + (1 - core), 0)
    arrived(opp * 2 + (1 - core), 1)
    gates(opp)
    gb_copy = pltpu.make_async_copy(gb, gb_out, osem.at[2])
    gb_copy.start()
    gather(opp, False)
    xs_copy = pltpu.make_async_copy(xs, xs_out, osem.at[3])
    xs_copy.start()
    for s in sends:
        s.wait_send()
    for i, peer in enumerate(others):
        pltpu.make_async_remote_copy(ids_ref, ids.at[me], ids_ssem.at[i], ids_rsem.at[me],
                                     device_id={'ep': peer}, device_id_type=MESH).wait_send()
    for cp in (tab_copy, pt_copy, gb_copy, xs_copy):
        cp.wait()


def hidden_kernel(nb, slots, ft, tab, xs_hbm, w1_hbm, w3_hbm, h_out, xs, w1, w3, h, xsem, wsem, hsem):
    e_local = w1_hbm.shape[0]
    ff = w1_hbm.shape[2]
    parts = ff // ft
    steps = e_local * parts
    used = tab[15, 0] + tab[7, 0]

    def wcopy(n):
        e, f = n // parts, n % parts
        slot = n % slots
        cols = pl.ds(pl.multiple_of(f * ft, ft), ft)
        return (pltpu.make_async_copy(w1_hbm.at[e, :, cols], w1.at[slot], wsem.at[0, slot]),
                pltpu.make_async_copy(w3_hbm.at[e, :, cols], w3.at[slot], wsem.at[1, slot]))

    def xcopy(b):
        rows = pl.ds(pl.multiple_of(b * BR, BR), BR)
        return pltpu.make_async_copy(xs_hbm.at[rows, :], xs.at[rows, :], xsem.at[b])

    for cp in wcopy(0):
        cp.start()

    @pl.loop(0, used)
    def _(b):
        xcopy(b).start()

    for n in range(1, slots):
        for cp in wcopy(n):
            cp.start()

    @pl.loop(used, nb)
    def _(b):
        h[pl.ds(pl.multiple_of(b * BR, BR), BR), :] = jnp.zeros((BR, ff), BF16)

    @pl.loop(0, steps)
    def _(n):
        e, f, slot = n // parts, n % parts, n % slots
        for cp in wcopy(n):
            cp.wait()
        first = tab[8 + e, 0]

        @pl.loop(first, first + tab[e, 0])
        def _(b):
            @pl.when(f == 0)
            def _():
                xcopy(b).wait()
            rows = pl.ds(pl.multiple_of(b * BR, BR), BR)
            xb = xs[rows, :]
            hg = jnp.dot(xb, w1[slot], preferred_element_type=F32)
            hu = jnp.dot(xb, w3[slot], preferred_element_type=F32)
            h[rows, pl.ds(pl.multiple_of(f * ft, ft), ft)] = (hg * jax.nn.sigmoid(hg) * hu).astype(BF16)

        @pl.when(n + slots < steps)
        def _():
            for cp in wcopy(n + slots):
                cp.start()

    out = pltpu.make_async_copy(h, h_out, hsem)
    out.start()
    out.wait()


def return_kernel(n_dev, nb, chunks, tab, x_ref, h_hbm, w2_hbm, pt_hbm, gb_hbm, o_ref,
                  h, w2a, w2b, pt, gb, o, dsend, drecv, z, r1, rd, r2, s2,
                  insem, wsem, d_ss, d_rs, s1_ss, r1_rs, rd_rs, s2_ss, r2_rs):
    me, chip, core, right, left, partner = ring_ids(n_dev)
    n_chip = n_dev // 2
    tok = x_ref.shape[0]
    half = tok // 2
    e_local = w2_hbm.shape[0]
    wait_entry = enter([right, left, partner])

    w2s = (w2a, w2b)

    def wcopy(k, i):
        return pltpu.make_async_copy(w2_hbm.at[:, :, pl.ds(pl.multiple_of(k * CW, CW), CW)], w2s[i], wsem.at[i])

    h_in = pltpu.make_async_copy(h_hbm, h, insem.at[0])
    h_in.start()
    wcopy(0, 0).start()
    pt_in = pltpu.make_async_copy(pt_hbm, pt, insem.at[1])
    pt_in.start()
    gb_in = pltpu.make_async_copy(gb_hbm, gb, insem.at[2])
    gb_in.start()
    o[nb * BR // ALIGN:] = jnp.zeros((o.shape[0] - nb * BR // ALIGN, ALIGN, CW), BF16)
    wait_entry()
    h_in.wait()

    lo, hi = pl.ds(0, half), pl.ds(half, half)
    rc, lc, oc = (chip + 1) % n_chip, (chip + n_chip - 1) % n_chip, (chip + 2) % n_chip

    def rcopy(src, dst, ss, rs, peer):
        return pltpu.make_async_remote_copy(src, dst, ss, rs, device_id={'ep': peer}, device_id_type=MESH)

    def pair_copy(k):
        return rcopy(dsend.at[k], drecv.at[k], d_ss.at[k], d_rs.at[k], partner)

    def s1_copies(k):
        return (rcopy(z.at[k, oc, lo, :], r1.at[k, 0], s1_ss.at[k, 0], r1_rs.at[k, 0], right),
                rcopy(z.at[k, oc, hi, :], r1.at[k, 1], s1_ss.at[k, 1], r1_rs.at[k, 1], left),
                rcopy(z.at[k, lc, lo, :], rd.at[k, 0], s1_ss.at[k, 2], rd_rs.at[k, 0], left),
                rcopy(z.at[k, rc, hi, :], rd.at[k, 1], s1_ss.at[k, 3], rd_rs.at[k, 1], right))

    def s2_copies(k):
        return (rcopy(s2.at[k, 0], r2.at[k, 0], s2_ss.at[k, 0], r2_rs.at[k, 0], right),
                rcopy(s2.at[k, 1], r2.at[k, 1], s2_ss.at[k, 1], r2_rs.at[k, 1], left))

    def combine(par, d):
        s = d * 2 + (core if par == 1 else 1 - core)
        acc = jnp.zeros((tok, CW), F32)
        for e in range(e_local):
            win = o[pl.ds(tab[24 + s * 8 + e, 0], WIN // ALIGN)].reshape(WIN, CW)
            m = jnp.dot(pt[par, d, e], win, preferred_element_type=F32)
            g = gb[par, d, e]
            acc = acc + jnp.concatenate([g] * (CW // 128), axis=1) * m
        return acc

    def one_step(k, i):
        @pl.when((k >= 5) & (k < chunks + 5))
        def _():
            kk = k - 5
            r2c, s1c = s2_copies(kk), s1_copies(kk)
            cols = pl.ds(pl.multiple_of(kk * CW, CW), CW)
            for i, rows in enumerate((lo, hi)):
                r2c[i].wait_recv()
                s1c[2 + i].wait_recv()
                tot = z[kk, chip, rows, :] + r2[kk, i] + rd[kk, i] + x_ref[rows, cols].astype(F32)
                o_ref[rows, cols] = tot.astype(BF16)

        @pl.when((k >= 3) & (k < chunks + 3))
        def _():
            kk = k - 3
            s1c, s2c = s1_copies(kk), s2_copies(kk)
            s1c[0].wait_recv()
            s2[kk, 0] = r1[kk, 0] + z[kk, rc, lo, :]
            s2c[0].start()
            s1c[1].wait_recv()
            s2[kk, 1] = r1[kk, 1] + z[kk, lc, hi, :]
            s2c[1].start()

        @pl.when(k < chunks)
        def _():
            wcopy(k, i).wait()

            @pl.when(k + 1 < chunks)
            def _():
                wcopy(k + 1, 1 - i).start()
            for b in range(nb):
                hb = h[b * BR:(b + 1) * BR, :]
                ob = jnp.dot(hb, w2s[i][tab[16, b]], preferred_element_type=F32).astype(BF16)
                o[b * BR // ALIGN:(b + 1) * BR // ALIGN] = ob.reshape(BR // ALIGN, ALIGN, CW)

        @pl.when((k >= 1) & (k < chunks + 1))
        def _():
            kk = k - 1
            pair_copy(kk).wait_recv()
            for d in range(n_chip):
                z[kk, d] = z[kk, d] + drecv[kk, d]
            for cp in s1_copies(kk):
                cp.start()

        @pl.when(k < chunks)
        def _():
            @pl.when(k == 0)
            def _():
                pt_in.wait()
                gb_in.wait()
            for d in range(n_chip):
                dsend[k, d] = combine(0, d)
            pair_copy(k).start()
            for d in range(n_chip):
                z[k, d] = combine(1, d)

    @pl.loop(0, (chunks + LAG + 1) // 2)
    def _(k2):
        one_step(k2 * 2, 0)
        one_step(k2 * 2 + 1, 1)

    @pl.loop(0, chunks)
    def _(k):
        pair_copy(k).wait_send()
        for cp in s1_copies(k) + s2_copies(k):
            cp.wait_send()


def solution(mesh):
    n_dev = mesh.shape['ep']

    def device_step(tokens, expert_ids, norm_gain, w_router, w_gate, w_up, w_down):
        tok, top_k = expert_ids.shape
        width = tokens.shape[1]
        e_local, _, ff = w_gate.shape
        n_chip = n_dev // 2
        recv_max = 3 * tok * top_k // 2
        nb = (recv_max - e_local) // BR + e_local
        rows = nb * BR
        chunks = width // CW
        me = lax.axis_index('ep')
        wr = jnp.roll(w_router, -me * e_local, axis=1)
        ids_t = expert_ids.T
        dma = pltpu.SemaphoreType.DMA
        params = lambda **kw: pltpu.CompilerParams(vmem_limit_bytes=60 * 1024 * 1024, **kw)

        xs, pt, gb, tab = pl.pallas_call(
            functools.partial(dispatch_kernel, n_dev, nb),
            name='dispatch',
            out_shape=(jax.ShapeDtypeStruct((rows, width), BF16),
                       jax.ShapeDtypeStruct((2, n_chip, e_local, tok, WIN), BF16),
                       jax.ShapeDtypeStruct((2, n_chip, e_local, tok, 128), F32),
                       jax.ShapeDtypeStruct((24 + n_dev * 8, 128), jnp.int32)),
            in_specs=[VM] * 4,
            out_specs=(ANY,) * 4,
            scratch_shapes=[pltpu.VMEM((n_dev, tok, width), BF16),
                            pltpu.VMEM((n_chip, rows, 2 * tok), BF16),
                            pltpu.VMEM((rows, width), BF16),
                            pltpu.VMEM((2, n_chip, e_local, tok, WIN), BF16),
                            pltpu.VMEM((2, n_chip, e_local, tok, 128), F32),
                            pltpu.VMEM((24 + n_dev * 8, 128), jnp.int32),
                            pltpu.VMEM((n_dev, top_k, tok), jnp.int32),
                            pltpu.VMEM((n_dev * 8, tok), F32),
                            dma((n_dev - 1,)), dma((n_dev,)), dma((14,)), dma((n_dev, 2)), dma((4,))],
            compiler_params=params(collective_id=0, has_side_effects=True),
        )(tokens, norm_gain.reshape(1, width), wr, ids_t)

        slots, ft = 3, 512
        h = pl.pallas_call(
            functools.partial(hidden_kernel, nb, slots, ft),
            name='hidden',
            out_shape=jax.ShapeDtypeStruct((rows, ff), BF16),
            in_specs=[SM, ANY, ANY, ANY],
            out_specs=ANY,
            scratch_shapes=[pltpu.VMEM((rows, width), BF16),
                            pltpu.VMEM((slots, width, ft), BF16),
                            pltpu.VMEM((slots, width, ft), BF16),
                            pltpu.VMEM((rows, ff), BF16),
                            dma((nb,)), dma((2, slots)), dma(())],
            compiler_params=params(),
        )(tab, xs, w_gate, w_up)

        blk = (chunks, 2, tok // 2, CW)
        out = pl.pallas_call(
            functools.partial(return_kernel, n_dev, nb, chunks),
            name='return',
            out_shape=jax.ShapeDtypeStruct((tok, width), BF16),
            in_specs=[SM, VM, ANY, ANY, ANY, ANY],
            out_specs=VM,
            scratch_shapes=[pltpu.VMEM((rows, ff), BF16),
                            pltpu.VMEM((e_local, ff, CW), BF16),
                            pltpu.VMEM((e_local, ff, CW), BF16),
                            pltpu.VMEM((2, n_chip, e_local, tok, WIN), BF16),
                            pltpu.VMEM((2, n_chip, e_local, tok, 128), F32),
                            pltpu.VMEM(((rows + WIN) // ALIGN, ALIGN, CW), BF16),
                            pltpu.VMEM((chunks, n_chip, tok, CW), F32),
                            pltpu.VMEM((chunks, n_chip, tok, CW), F32),
                            pltpu.VMEM((chunks, n_chip, tok, CW), F32),
                            pltpu.VMEM(blk, F32), pltpu.VMEM(blk, F32), pltpu.VMEM(blk, F32), pltpu.VMEM(blk, F32),
                            dma((3,)), dma((2,)), dma((chunks,)), dma((chunks,)),
                            dma((chunks, 4)), dma((chunks, 2)), dma((chunks, 2)), dma((chunks, 2)), dma((chunks, 2))],
            compiler_params=params(collective_id=1, has_side_effects=True),
        )(tab, tokens, h, w_down, pt, gb)
        return out

    row_spec = P(('dp', 'ep'), None)
    expert_spec = P('ep', None, None)
    return jax.shard_map(device_step, mesh=mesh, in_specs=(row_spec, row_spec, P(None), P(None, None), expert_spec, expert_spec, expert_spec), out_specs=row_spec, check_vma=False)
```

```python
import functools

import jax
import jax.numpy as jnp
from jax import lax
from jax.experimental import pallas as pl
from jax.experimental.pallas import tpu as pltpu
from jax.sharding import PartitionSpec as P

NORM_EPS = 1e-5
BR = 128
WIN = 256
ALIGN = 16
FC = 128
CW = 256
LAG = 5
F32 = jnp.float32
BF16 = jnp.bfloat16
I32 = jnp.int32
MESH = pl.DeviceIdType.MESH
ANY = pl.BlockSpec(memory_space=pl.ANY)
VM = pl.BlockSpec(memory_space=pltpu.VMEM)


def moe_kernel(n_dev, nb, chunks, x_ref, ids_ref, g_ref, wr_ref, w1_hbm, w3_hbm, w2_hbm, o_ref,
               u, wb0, wb1, h, pt, gb, ids, posm, tab_v, tab, drecv, r1, rd, r2,
               wsem, tsem, ids_ssem, ids_rsem, ssem, rsem,
               d_ss, d_rs, s1_ss, r1_rs, rd_rs, s2_ss, r2_rs):
    n_chip = n_dev // 2
    tok, width = x_ref.shape
    half = tok // 2
    top_k = ids_ref.shape[0]
    e_local, ff = w2_hbm.shape[0], w2_hbm.shape[1]
    rows = nb * BR
    f_steps = ff // FC
    wbs = (wb0, wb1)

    def rcopy(src, dst, ss, rs, peer):
        return pltpu.make_async_remote_copy(src, dst, ss, rs, device_id={'ep': peer}, device_id_type=MESH)

    def expert_of(b):
        return jnp.minimum(jnp.maximum(tab[0, b], 0), e_local - 1)

    def window_of(s, e):
        return jnp.minimum(jnp.maximum(tab[8 + s * 8 + e, 0], 0), rows // ALIGN)

    def coords():
        me = lax.axis_index('ep')
        chip, core = me // 2, me % 2
        rc, lc, oc = (chip + 1) % n_chip, (chip + n_chip - 1) % n_chip, (chip + 2) % n_chip
        return me, chip, core, rc, lc, oc, rc * 2 + core, lc * 2 + core, chip * 2 + (1 - core)

    def hidden_copies(f, i):
        cols = pl.ds(pl.multiple_of(f * FC, FC), FC)
        return (pltpu.make_async_copy(w1_hbm.at[:, :, cols], wbs[i].at[:, :, 0:FC], wsem.at[0, i]),
                pltpu.make_async_copy(w3_hbm.at[:, :, cols], wbs[i].at[:, :, FC:2 * FC], wsem.at[1, i]))

    def down_copy(k, i):
        return pltpu.make_async_copy(w2_hbm.at[:, :, pl.ds(pl.multiple_of(k * CW, CW), CW)],
                                     wbs[i].at[:, 0:ff, :], wsem.at[2, i])

    def dispatch(p, xs):
        me, chip, core, rc, lc, oc, right, left, partner = coords()
        others = [(me + i) % n_dev for i in range(1, n_dev)]
        barrier = pltpu.get_barrier_semaphore()
        for peer in others:
            pl.semaphore_signal(barrier, inc=1, device_id={'ep': peer}, device_id_type=MESH)

        for i in range(2):
            for cp in hidden_copies(i, i):
                cp.start()

        gain = g_ref[...].astype(F32).reshape(1, width)
        step = tok // 4
        for i in range(4):
            x32 = x_ref[i * step:(i + 1) * step, :].astype(F32)
            inv = lax.rsqrt(jnp.mean(x32 * x32, axis=1, keepdims=True) + NORM_EPS)
            u[chip, pl.ds(pl.multiple_of(core * tok + i * step, step), step), :] = (x32 * inv * gain).astype(BF16)
        pl.semaphore_wait(barrier, n_dev - 1)

        def send(i, blk, hf, peer):
            ref = u.at[blk // 2, pl.ds(pl.multiple_of((blk % 2) * tok + hf * half, half), half), :]
            return rcopy(ref, ref, ssem.at[i], rsem.at[blk, hf], peer)

        def ids_send(i, peer):
            return rcopy(ids_ref, ids.at[me], ids_ssem.at[i], ids_rsem.at[me], peer)

        for i, peer in enumerate(others):
            ids_send(i, peer).start()
        sends = [send(0, me, 0, right), send(1, me, 1, left), send(2, me, 0, partner), send(3, me, 1, partner),
                 send(4, me, 1, right), send(5, me, 0, left)]
        for s in sends:
            s.start()

        def arrived(blk, hf):
            send(0, blk, hf, partner).wait_recv()

        def forward(i, blk, hf, peer):
            s = send(i, blk, hf, peer)
            s.start()
            sends.append(s)

        ids[me] = ids_ref[...]
        for i in range(1, n_dev):
            src = (me + i) % n_dev
            rcopy(ids_ref, ids.at[src], ids_ssem.at[0], ids_rsem.at[src], partner).wait_recv()
        sub = lax.broadcasted_iota(I32, (e_local, tok), 0)
        gid = sub + me * e_local
        hits = []
        for s in range(n_dev):
            hit = jnp.zeros((e_local, tok), I32)
            for j in range(top_k):
                hit = hit + (ids[s, j:j + 1, :] == gid).astype(I32)
            hits.append(hit.astype(F32))
        hit_all = jnp.concatenate(hits, axis=0).astype(BF16)
        ri = lax.broadcasted_iota(I32, (tok, tok), 0)
        ci = lax.broadcasted_iota(I32, (tok, tok), 1)
        before = (ri < ci).astype(F32).astype(BF16)
        cnt_all = jnp.dot(hit_all, jnp.ones((tok, tok), BF16), preferred_element_type=F32)
        rank_all = jnp.dot(hit_all, before, preferred_element_type=F32)
        total = jnp.zeros((e_local, tok), F32)
        for s in range(n_dev):
            total = total + cnt_all[s * e_local:(s + 1) * e_local, :]
        blocks = jnp.floor((total + (BR - 1)) * (1.0 / BR))
        first = jnp.zeros((e_local, tok), F32)
        for e in range(e_local - 1):
            first = first + jnp.where(sub > e, jnp.broadcast_to(blocks[e:e + 1, :], (e_local, tok)), 0.0)
        last = first + blocks
        lane = lax.broadcasted_iota(I32, (e_local, tok), 1).astype(F32)
        blk_exp = jnp.sum(jnp.where(lane >= last, 1.0, 0.0), axis=0, keepdims=True)
        tab_v[0:8, :] = jnp.broadcast_to(jnp.minimum(blk_exp, e_local - 1.0), (8, tok)).astype(I32)
        carry = jnp.zeros((e_local, tok), F32)
        starts, rels = [], []
        for s in range(n_dev):
            run = first * BR + carry
            pos = run + rank_all[s * e_local:(s + 1) * e_local, :]
            start = jnp.floor(run * (1.0 / ALIGN))
            tab_v[8 + s * 8:16 + s * 8, :] = jnp.minimum(start, 1.0 * (rows // ALIGN)).astype(I32)
            rels.append(jnp.where(hits[s] > 0, pos - start * ALIGN, -1.0))
            posm[s * 8:(s + 1) * 8, :] = jnp.where(hits[s] > 0, pos + 1.0, 0.0)
            carry = carry + cnt_all[s * e_local:(s + 1) * e_local, :]
        tab_copy = pltpu.make_async_copy(tab_v, tab, tsem)
        tab_copy.start()
        row_i = lax.broadcasted_iota(I32, (BR, tok), 0).astype(F32)

        @pl.loop(0, nb)
        def _(b):
            bf = b.astype(F32)
            mine = (first <= bf) & (bf < last)
            for s in range(n_dev):
                sel = jnp.sum(jnp.where(mine, posm[s * 8:(s + 1) * 8, :], 0.0), axis=0, keepdims=True) - (1.0 + BR * bf)
                p[s // 2, pl.ds(pl.multiple_of(b * BR, BR), BR), (s % 2) * tok:(s % 2 + 1) * tok] = jnp.where(
                    jnp.broadcast_to(sel, (BR, tok)) == row_i, 1.0, 0.0).astype(BF16)

        def windows():
            wlane = lax.broadcasted_iota(I32, (tok, WIN), 1).astype(F32)
            for s in range(n_dev):
                rel_t = jnp.concatenate([rels[s], jnp.zeros((tok - e_local, tok), F32)], axis=0).T
                par = (s % 2 + core + 1) % 2
                for e in range(e_local):
                    col = jnp.broadcast_to(rel_t[:, e:e + 1], (tok, WIN))
                    pt[par, s // 2, e] = jnp.where(col == wlane, 1.0, 0.0).astype(BF16)

        def gates(c):
            logits = lax.dot_general(u[c], wr_ref[...], (((1,), (1,)), ((), ())), preferred_element_type=F32)
            ex = jnp.exp(logits - jnp.max(logits, axis=1, keepdims=True))
            prob = ex / jnp.sum(ex, axis=1, keepdims=True)
            full = jnp.concatenate([prob, jnp.zeros((2 * tok, 128 - prob.shape[1]), F32)], axis=1)
            mine = pltpu.roll(full, (128 - me * e_local) % 128, 1)
            for k in range(2):
                par = (k + core + 1) % 2
                for e in range(e_local):
                    gb[par, c, e] = jnp.broadcast_to(mine[k * tok:(k + 1) * tok, e:e + 1], (tok, 128))

        mt, nt = rows // 4, 256

        def gather(cs, first_pass):
            @pl.loop(0, rows // mt)
            def _(m):
                rs = pl.ds(pl.multiple_of(m * mt, mt), mt)
                for n in range(width // nt):
                    cols = slice(n * nt, (n + 1) * nt)
                    part = jnp.dot(p[cs[0], rs, :], u[cs[0], :, cols], preferred_element_type=F32)
                    for c in cs[1:]:
                        part = part + jnp.dot(p[c, rs, :], u[c, :, cols], preferred_element_type=F32)
                    if first_pass:
                        xs[rs, cols] = part.astype(BF16)
                    else:
                        xs[rs, cols] = xs[rs, cols] + part.astype(BF16)

        arrived(partner, 0)
        arrived(partner, 1)
        arrived(left, 0)
        forward(6, left, 0, right)
        arrived(right, 1)
        forward(7, right, 1, left)
        forward(8, left, 0, partner)
        forward(9, right, 1, partner)
        gather([chip], True)
        gates(chip)
        arrived(left, 1)
        forward(10, left, 1, partner)
        arrived(right, 0)
        forward(11, right, 0, partner)
        windows()
        for blk in (lc * 2 + (1 - core), rc * 2 + (1 - core)):
            arrived(blk, 0)
            arrived(blk, 1)
        gather([lc, rc], False)
        oblk = oc * 2 + core
        arrived(oblk, 0)
        forward(12, oblk, 0, partner)
        arrived(oblk, 1)
        forward(13, oblk, 1, partner)
        gates(lc)
        gates(rc)
        arrived(oc * 2 + (1 - core), 0)
        arrived(oc * 2 + (1 - core), 1)
        gather([oc], False)
        gates(oc)
        tab_copy.wait()

        @pl.loop(0, f_steps // 2)
        def _(f2):
            for i in range(2):
                f = f2 * 2 + i
                for cp in hidden_copies(f, i):
                    cp.wait()
                for b in range(nb):
                    r = jnp.dot(xs[b * BR:(b + 1) * BR, :], wbs[i][expert_of(b)], preferred_element_type=F32)
                    hg, hu = r[:, 0:FC], r[:, FC:2 * FC]
                    h[b * BR:(b + 1) * BR, pl.ds(pl.multiple_of(f * FC, FC), FC)] = (hg * jax.nn.sigmoid(hg) * hu).astype(BF16)

                @pl.when(f + 2 < f_steps)
                def _():
                    for cp in hidden_copies(f + 2, i):
                        cp.start()

                @pl.when(f + 2 >= f_steps)
                def _():
                    down_copy(i, i).start()

        for s in sends:
            s.wait_send()
        for i, peer in enumerate(others):
            ids_send(i, peer).wait_send()

    pl.run_scoped(dispatch, pltpu.VMEM((n_chip, rows, 2 * tok), BF16), pltpu.VMEM((rows, width), BF16))

    lo, hi = pl.ds(0, half), pl.ds(half, half)

    def give_back(o, dsend, z, s2):
        _, chip, core, rc, lc, oc, right, left, partner = coords()

        def pair_copy(k):
            return rcopy(dsend.at[k], drecv.at[k], d_ss.at[k], d_rs.at[k], partner)

        def s1_copies(k):
            return (rcopy(z.at[k, oc, lo, :], r1.at[k, 0], s1_ss.at[k, 0], r1_rs.at[k, 0], right),
                    rcopy(z.at[k, oc, hi, :], r1.at[k, 1], s1_ss.at[k, 1], r1_rs.at[k, 1], left),
                    rcopy(z.at[k, lc, lo, :], rd.at[k, 0], s1_ss.at[k, 2], rd_rs.at[k, 0], left),
                    rcopy(z.at[k, rc, hi, :], rd.at[k, 1], s1_ss.at[k, 3], rd_rs.at[k, 1], right))

        def s2_copies(k):
            return (rcopy(s2.at[k, 0], r2.at[k, 0], s2_ss.at[k, 0], r2_rs.at[k, 0], right),
                    rcopy(s2.at[k, 1], r2.at[k, 1], s2_ss.at[k, 1], r2_rs.at[k, 1], left))

        def combine(par, d):
            s = d * 2 + (core if par == 1 else 1 - core)
            acc = jnp.zeros((tok, CW), F32)
            for e in range(e_local):
                win = o[pl.ds(window_of(s, e), WIN // ALIGN)].reshape(WIN, CW)
                m = jnp.dot(pt[par, d, e], win, preferred_element_type=F32)
                acc = acc + jnp.concatenate([gb[par, d, e]] * (CW // 128), axis=1) * m
            return acc

        def one_step(k, i):
            @pl.when((k >= 5) & (k < chunks + 5))
            def _():
                kk = k - 5
                r2c, s1c = s2_copies(kk), s1_copies(kk)
                cols = pl.ds(pl.multiple_of(kk * CW, CW), CW)
                for j, rs in enumerate((lo, hi)):
                    r2c[j].wait_recv()
                    s1c[2 + j].wait_recv()
                    tot = z[kk, chip, rs, :] + r2[kk, j] + rd[kk, j] + x_ref[rs, cols].astype(F32)
                    o_ref[rs, cols] = tot.astype(BF16)

            @pl.when((k >= 3) & (k < chunks + 3))
            def _():
                kk = k - 3
                s1c, s2c = s1_copies(kk), s2_copies(kk)
                s1c[0].wait_recv()
                s2[kk, 0] = r1[kk, 0] + z[kk, rc, lo, :]
                s2c[0].start()
                s1c[1].wait_recv()
                s2[kk, 1] = r1[kk, 1] + z[kk, lc, hi, :]
                s2c[1].start()

            @pl.when(k < chunks)
            def _():
                down_copy(k, i).wait()
                for b in range(nb):
                    ob = jnp.dot(h[b * BR:(b + 1) * BR, :], wbs[i][expert_of(b), 0:ff, :], preferred_element_type=F32)
                    o[b * BR // ALIGN:(b + 1) * BR // ALIGN] = ob.astype(BF16).reshape(BR // ALIGN, ALIGN, CW)

            @pl.when(k + 2 < chunks)
            def _():
                down_copy(k + 2, i).start()

            @pl.when((k >= 1) & (k < chunks + 1))
            def _():
                kk = k - 1
                pair_copy(kk).wait_recv()
                for d in range(n_chip):
                    z[kk, d] = z[kk, d] + drecv[kk, d]
                for cp in s1_copies(kk):
                    cp.start()

            @pl.when(k < chunks)
            def _():
                for d in range(n_chip):
                    dsend[k, d] = combine(0, d)
                pair_copy(k).start()
                for d in range(n_chip):
                    z[k, d] = combine(1, d)

        o[rows // ALIGN:] = jnp.zeros((WIN // ALIGN, ALIGN, CW), BF16)

        @pl.loop(0, (chunks + LAG + 1) // 2)
        def _(k2):
            one_step(k2 * 2, 0)
            one_step(k2 * 2 + 1, 1)

        @pl.loop(0, chunks)
        def _(k):
            pair_copy(k).wait_send()
            for cp in s1_copies(k) + s2_copies(k):
                cp.wait_send()

    pl.run_scoped(give_back, pltpu.VMEM(((rows + WIN) // ALIGN, ALIGN, CW), BF16),
                  pltpu.VMEM((chunks, n_chip, tok, CW), F32), pltpu.VMEM((chunks, n_chip, tok, CW), F32),
                  pltpu.VMEM((chunks, 2, half, CW), F32))


def solution(mesh):
    n_dev = mesh.shape['ep']

    def device_step(tokens, expert_ids, norm_gain, w_router, w_gate, w_up, w_down):
        tok, top_k = expert_ids.shape
        width = tokens.shape[1]
        e_local, _, ff = w_gate.shape
        n_chip = n_dev // 2
        recv_max = 3 * tok * top_k // 2
        nb = (recv_max - e_local) // BR + e_local
        rows = nb * BR
        chunks = width // CW
        dma = pltpu.SemaphoreType.DMA
        half_blk = (chunks, 2, tok // 2, CW)
        tabs = (8 + n_dev * 8, 128)
        wbuf = pltpu.VMEM((e_local, width, 2 * FC), BF16)
        return pl.pallas_call(
            functools.partial(moe_kernel, n_dev, nb, chunks),
            name='moe',
            out_shape=jax.ShapeDtypeStruct((tok, width), BF16),
            in_specs=[VM] * 4 + [ANY] * 3,
            out_specs=VM,
            scratch_shapes=[pltpu.VMEM((n_chip, 2 * tok, width), BF16), wbuf, wbuf,
                            pltpu.VMEM((rows, ff), BF16),
                            pltpu.VMEM((2, n_chip, e_local, tok, WIN), BF16),
                            pltpu.VMEM((2, n_chip, e_local, tok, 128), F32),
                            pltpu.VMEM((n_dev, top_k, tok), I32),
                            pltpu.VMEM((n_dev * 8, tok), F32),
                            pltpu.VMEM(tabs, I32), pltpu.SMEM(tabs, I32),
                            pltpu.VMEM((chunks, n_chip, tok, CW), F32),
                            pltpu.VMEM(half_blk, F32), pltpu.VMEM(half_blk, F32), pltpu.VMEM(half_blk, F32),
                            dma((3, 2)), dma(()), dma((n_dev - 1,)), dma((n_dev,)), dma((14,)), dma((n_dev, 2)),
                            dma((chunks,)), dma((chunks,)),
                            dma((chunks, 4)), dma((chunks, 2)), dma((chunks, 2)), dma((chunks, 2)), dma((chunks, 2))],
            compiler_params=pltpu.CompilerParams(vmem_limit_bytes=67043328, collective_id=0, has_side_effects=True),
        )(tokens, expert_ids.T, norm_gain, w_router.T, w_gate, w_up, w_down)

    row_spec = P(('dp', 'ep'), None)
    expert_spec = P('ep', None, None)
    return jax.shard_map(device_step, mesh=mesh, in_specs=(row_spec, row_spec, P(None), P(None, None), expert_spec, expert_spec, expert_spec), out_specs=row_spec, check_vma=False)
```

```python
import functools

import jax
import jax.numpy as jnp
from jax import lax
from jax.experimental import pallas as pl
from jax.experimental.pallas import tpu as pltpu
from jax.sharding import PartitionSpec as P

NORM_EPS = 1e-5
BR = 128
WIN = 256
ALIGN = 16
FC = 128
CW = 256
LAG = 5
F32 = jnp.float32
BF16 = jnp.bfloat16
I32 = jnp.int32
MESH = pl.DeviceIdType.MESH
ANY = pl.BlockSpec(memory_space=pl.ANY)
VM = pl.BlockSpec(memory_space=pltpu.VMEM)


def moe_kernel(n_dev, nb, chunks, x_ref, ids_ref, g_ref, wr_ref, w1_hbm, w3_hbm, w2_hbm, o_ref,
               u, wb0, wb1, h, pt, gb, ids, posm, tab_v, tab, drecv, r1, rd, r2,
               wsem, tsem, ids_ssem, ids_rsem, ssem, rsem,
               d_ss, d_rs, s1_ss, r1_rs, rd_rs, s2_ss, r2_rs):
    n_chip = n_dev // 2
    tok, width = x_ref.shape
    half = tok // 2
    top_k = ids_ref.shape[0]
    e_local, ff = w2_hbm.shape[0], w2_hbm.shape[1]
    rows = nb * BR
    f_steps = ff // FC
    wbs = (wb0, wb1)

    def rcopy(src, dst, ss, rs, peer):
        return pltpu.make_async_remote_copy(src, dst, ss, rs, device_id={'ep': peer}, device_id_type=MESH)

    def expert_of(b):
        return jnp.minimum(jnp.maximum(tab[0, b], 0), e_local - 1)

    def window_of(s, e):
        return jnp.minimum(jnp.maximum(tab[8 + s * 8 + e, 0], 0), rows // ALIGN)

    def coords():
        me = lax.axis_index('ep')
        chip, core = me // 2, me % 2
        rc, lc, oc = (chip + 1) % n_chip, (chip + n_chip - 1) % n_chip, (chip + 2) % n_chip
        return me, chip, core, rc, lc, oc, rc * 2 + core, lc * 2 + core, chip * 2 + (1 - core)

    def hidden_copies(f, i):
        cols = pl.ds(pl.multiple_of(f * FC, FC), FC)
        return (pltpu.make_async_copy(w1_hbm.at[:, :, cols], wbs[i].at[:, :, 0:FC], wsem.at[0, i]),
                pltpu.make_async_copy(w3_hbm.at[:, :, cols], wbs[i].at[:, :, FC:2 * FC], wsem.at[1, i]))

    def down_copy(k, i):
        return pltpu.make_async_copy(w2_hbm.at[:, :, pl.ds(pl.multiple_of(k * CW, CW), CW)],
                                     wbs[i].at[:, 0:ff, :], wsem.at[2, i])

    def dispatch(p, xs):
        me, chip, core, rc, lc, oc, right, left, partner = coords()
        others = [(me + i) % n_dev for i in range(1, n_dev)]
        barrier = pltpu.get_barrier_semaphore()
        for peer in others:
            pl.semaphore_signal(barrier, inc=1, device_id={'ep': peer}, device_id_type=MESH)

        for i in range(2):
            for cp in hidden_copies(i, i):
                cp.start()

        gain = g_ref[...].astype(F32).reshape(1, width)
        step = tok // 4
        for i in range(4):
            x32 = x_ref[i * step:(i + 1) * step, :].astype(F32)
            inv = lax.rsqrt(jnp.mean(x32 * x32, axis=1, keepdims=True) + NORM_EPS)
            u[chip, pl.ds(pl.multiple_of((i // 2) * tok + core * half + (i % 2) * step, step), step), :] = (x32 * inv * gain).astype(BF16)
        pl.semaphore_wait(barrier, n_dev - 1)

        def send(i, blk, hf, peer):
            ref = u.at[blk // 2, pl.ds(pl.multiple_of(hf * tok + (blk % 2) * half, half), half), :]
            return rcopy(ref, ref, ssem.at[i], rsem.at[blk, hf], peer)

        def ids_send(i, peer):
            return rcopy(ids_ref, ids.at[me], ids_ssem.at[i], ids_rsem.at[me], peer)

        for i, peer in enumerate(others):
            ids_send(i, peer).start()
        sends = [send(0, me, 0, right), send(1, me, 1, left), send(2, me, 0, partner), send(3, me, 1, partner),
                 send(4, me, 1, right), send(5, me, 0, left)]
        for s in sends:
            s.start()

        def arrived(blk, hf):
            send(0, blk, hf, partner).wait_recv()

        def forward(i, blk, hf, peer):
            s = send(i, blk, hf, peer)
            s.start()
            sends.append(s)

        ids[me] = ids_ref[...]
        for i in range(1, n_dev):
            src = (me + i) % n_dev
            rcopy(ids_ref, ids.at[src], ids_ssem.at[0], ids_rsem.at[src], partner).wait_recv()
        sub = lax.broadcasted_iota(I32, (e_local, tok), 0)
        gid = sub + me * e_local
        hits = []
        for s in range(n_dev):
            hit = jnp.zeros((e_local, tok), I32)
            for j in range(top_k):
                hit = hit + (ids[s, j:j + 1, :] == gid).astype(I32)
            hits.append(hit.astype(F32))
        hit_all = jnp.concatenate(hits, axis=0).astype(BF16)
        ri = lax.broadcasted_iota(I32, (tok, tok), 0)
        ci = lax.broadcasted_iota(I32, (tok, tok), 1)
        before = (ri < ci).astype(F32).astype(BF16)
        cnt_all = jnp.dot(hit_all, jnp.ones((tok, tok), BF16), preferred_element_type=F32)
        rank_all = jnp.dot(hit_all, before, preferred_element_type=F32)
        total = jnp.zeros((e_local, tok), F32)
        for s in range(n_dev):
            total = total + cnt_all[s * e_local:(s + 1) * e_local, :]
        blocks = jnp.floor((total + (BR - 1)) * (1.0 / BR))
        first = jnp.zeros((e_local, tok), F32)
        for e in range(e_local - 1):
            first = first + jnp.where(sub > e, jnp.broadcast_to(blocks[e:e + 1, :], (e_local, tok)), 0.0)
        last = first + blocks
        lane = lax.broadcasted_iota(I32, (e_local, tok), 1).astype(F32)
        blk_exp = jnp.sum(jnp.where(lane >= last, 1.0, 0.0), axis=0, keepdims=True)
        tab_v[0:8, :] = jnp.broadcast_to(jnp.minimum(blk_exp, e_local - 1.0), (8, tok)).astype(I32)
        carry = jnp.zeros((e_local, tok), F32)
        starts, rels = [], []
        for s in range(n_dev):
            run = first * BR + carry
            pos = run + rank_all[s * e_local:(s + 1) * e_local, :]
            start = jnp.floor(run * (1.0 / ALIGN))
            tab_v[8 + s * 8:16 + s * 8, :] = jnp.minimum(start, 1.0 * (rows // ALIGN)).astype(I32)
            rels.append(jnp.where(hits[s] > 0, pos - start * ALIGN, -1.0))
            posm[s * 8:(s + 1) * 8, :] = jnp.where(hits[s] > 0, pos + 1.0, 0.0)
            carry = carry + cnt_all[s * e_local:(s + 1) * e_local, :]
        tab_copy = pltpu.make_async_copy(tab_v, tab, tsem)
        tab_copy.start()
        row_i = lax.broadcasted_iota(I32, (BR, tok), 0).astype(F32)

        @pl.loop(0, nb)
        def _(b):
            bf = b.astype(F32)
            mine = (first <= bf) & (bf < last)
            rs = pl.ds(pl.multiple_of(b * BR, BR), BR)
            sel = [jnp.sum(jnp.where(mine, posm[s * 8:(s + 1) * 8, :], 0.0), axis=0, keepdims=True) - (1.0 + BR * bf)
                   for s in range(n_dev)]
            for c in range(n_chip):
                for hf in range(2):
                    cut = slice(hf * half, (hf + 1) * half)
                    both = jnp.concatenate([sel[2 * c][:, cut], sel[2 * c + 1][:, cut]], axis=1)
                    p[c, rs, hf * tok:(hf + 1) * tok] = jnp.where(
                        jnp.broadcast_to(both, (BR, tok)) == row_i, 1.0, 0.0).astype(BF16)

        def windows():
            wlane = lax.broadcasted_iota(I32, (tok, WIN), 1).astype(F32)
            for s in range(n_dev):
                rel_t = jnp.concatenate([rels[s], jnp.zeros((tok - e_local, tok), F32)], axis=0).T
                par = (s % 2 + core + 1) % 2
                for e in range(e_local):
                    col = jnp.broadcast_to(rel_t[:, e:e + 1], (tok, WIN))
                    pt[par, s // 2, e] = jnp.where(col == wlane, 1.0, 0.0).astype(BF16)

        def gates(c):
            logits = lax.dot_general(u[c], wr_ref[...], (((1,), (1,)), ((), ())), preferred_element_type=F32)
            ex = jnp.exp(logits - jnp.max(logits, axis=1, keepdims=True))
            prob = ex / jnp.sum(ex, axis=1, keepdims=True)
            full = jnp.concatenate([prob, jnp.zeros((2 * tok, 128 - prob.shape[1]), F32)], axis=1)
            mine = pltpu.roll(full, (128 - me * e_local) % 128, 1)
            for k in range(2):
                par = (k + core + 1) % 2
                own = jnp.concatenate([mine[k * half:(k + 1) * half], mine[tok + k * half:tok + (k + 1) * half]], axis=0)
                for e in range(e_local):
                    gb[par, c, e] = jnp.broadcast_to(own[:, e:e + 1], (tok, 128))

        mt, nt = rows // 4, 256

        def gather(pieces, first_pass):
            @pl.loop(0, rows // mt)
            def _(m):
                rs = pl.ds(pl.multiple_of(m * mt, mt), mt)
                pick = [p[c, rs, a:b] for c, a, b in pieces]
                pick = pick[0] if len(pick) == 1 else jnp.concatenate(pick, axis=1)
                for n in range(width // nt):
                    cols = slice(n * nt, (n + 1) * nt)
                    tile = [u[c, a:b, cols] for c, a, b in pieces]
                    tile = tile[0] if len(tile) == 1 else jnp.concatenate(tile, axis=0)
                    part = jnp.dot(pick, tile, preferred_element_type=F32).astype(BF16)
                    if first_pass:
                        xs[rs, cols] = part
                    else:
                        xs[rs, cols] = xs[rs, cols] + part

        l_other, r_other, o_own, o_other = lc * 2 + (1 - core), rc * 2 + (1 - core), oc * 2 + core, oc * 2 + (1 - core)
        arrived(partner, 0)
        arrived(partner, 1)
        gather([(chip, 0, 2 * tok)], True)
        arrived(left, 0)
        forward(6, left, 0, right)
        arrived(right, 1)
        forward(7, right, 1, left)
        forward(8, left, 0, partner)
        forward(9, right, 1, partner)
        windows()
        gates(chip)
        arrived(l_other, 0)
        arrived(r_other, 1)
        gather([(lc, 0, tok), (rc, tok, 2 * tok)], False)
        arrived(left, 1)
        forward(10, left, 1, partner)
        arrived(right, 0)
        forward(11, right, 0, partner)
        arrived(l_other, 1)
        arrived(r_other, 0)
        gather([(lc, tok, 2 * tok), (rc, 0, tok)], False)
        arrived(o_own, 0)
        forward(12, o_own, 0, partner)
        arrived(o_own, 1)
        forward(13, o_own, 1, partner)
        gates(lc)
        gates(rc)
        arrived(o_other, 0)
        arrived(o_other, 1)
        gather([(oc, 0, 2 * tok)], False)
        gates(oc)
        tab_copy.wait()

        @pl.loop(0, f_steps // 2)
        def _(f2):
            for i in range(2):
                f = f2 * 2 + i
                for cp in hidden_copies(f, i):
                    cp.wait()
                for b in range(nb):
                    r = jnp.dot(xs[b * BR:(b + 1) * BR, :], wbs[i][expert_of(b)], preferred_element_type=F32)
                    hg, hu = r[:, 0:FC], r[:, FC:2 * FC]
                    h[b * BR:(b + 1) * BR, pl.ds(pl.multiple_of(f * FC, FC), FC)] = (hg * jax.nn.sigmoid(hg) * hu).astype(BF16)

                @pl.when(f + 2 < f_steps)
                def _():
                    for cp in hidden_copies(f + 2, i):
                        cp.start()

                @pl.when(f + 2 >= f_steps)
                def _():
                    down_copy(i, i).start()

        for s in sends:
            s.wait_send()
        for i, peer in enumerate(others):
            ids_send(i, peer).wait_send()

    pl.run_scoped(dispatch, pltpu.VMEM((n_chip, rows, 2 * tok), BF16), pltpu.VMEM((rows, width), BF16))

    lo, hi = pl.ds(0, half), pl.ds(half, half)

    def give_back(o, dsend, z, s2):
        _, chip, core, rc, lc, oc, right, left, partner = coords()

        def pair_copy(k):
            return rcopy(dsend.at[k], drecv.at[k], d_ss.at[k], d_rs.at[k], partner)

        def s1_copies(k):
            return (rcopy(z.at[k, oc, lo, :], r1.at[k, 0], s1_ss.at[k, 0], r1_rs.at[k, 0], right),
                    rcopy(z.at[k, oc, hi, :], r1.at[k, 1], s1_ss.at[k, 1], r1_rs.at[k, 1], left),
                    rcopy(z.at[k, lc, lo, :], rd.at[k, 0], s1_ss.at[k, 2], rd_rs.at[k, 0], left),
                    rcopy(z.at[k, rc, hi, :], rd.at[k, 1], s1_ss.at[k, 3], rd_rs.at[k, 1], right))

        def s2_copies(k):
            return (rcopy(s2.at[k, 0], r2.at[k, 0], s2_ss.at[k, 0], r2_rs.at[k, 0], right),
                    rcopy(s2.at[k, 1], r2.at[k, 1], s2_ss.at[k, 1], r2_rs.at[k, 1], left))

        def combine(par, d):
            s = d * 2 + (core if par == 1 else 1 - core)
            acc = jnp.zeros((tok, CW), F32)
            for e in range(e_local):
                win = o[pl.ds(window_of(s, e), WIN // ALIGN)].reshape(WIN, CW)
                m = jnp.dot(pt[par, d, e], win, preferred_element_type=F32)
                acc = acc + jnp.concatenate([gb[par, d, e]] * (CW // 128), axis=1) * m
            return acc

        def one_step(k, i):
            @pl.when((k >= 5) & (k < chunks + 5))
            def _():
                kk = k - 5
                r2c, s1c = s2_copies(kk), s1_copies(kk)
                cols = pl.ds(pl.multiple_of(kk * CW, CW), CW)
                for j, rs in enumerate((lo, hi)):
                    r2c[j].wait_recv()
                    s1c[2 + j].wait_recv()
                    tot = z[kk, chip, rs, :] + r2[kk, j] + rd[kk, j] + x_ref[rs, cols].astype(F32)
                    o_ref[rs, cols] = tot.astype(BF16)

            @pl.when((k >= 3) & (k < chunks + 3))
            def _():
                kk = k - 3
                s1c, s2c = s1_copies(kk), s2_copies(kk)
                s1c[0].wait_recv()
                s2[kk, 0] = r1[kk, 0] + z[kk, rc, lo, :]
                s2c[0].start()
                s1c[1].wait_recv()
                s2[kk, 1] = r1[kk, 1] + z[kk, lc, hi, :]
                s2c[1].start()

            @pl.when(k < chunks)
            def _():
                down_copy(k, i).wait()
                for b in range(nb):
                    ob = jnp.dot(h[b * BR:(b + 1) * BR, :], wbs[i][expert_of(b), 0:ff, :], preferred_element_type=F32)
                    o[b * BR // ALIGN:(b + 1) * BR // ALIGN] = ob.astype(BF16).reshape(BR // ALIGN, ALIGN, CW)

            @pl.when(k + 2 < chunks)
            def _():
                down_copy(k + 2, i).start()

            @pl.when((k >= 1) & (k < chunks + 1))
            def _():
                kk = k - 1
                pair_copy(kk).wait_recv()
                for d in range(n_chip):
                    z[kk, d] = z[kk, d] + drecv[kk, d]
                for cp in s1_copies(kk):
                    cp.start()

            @pl.when(k < chunks)
            def _():
                for d in range(n_chip):
                    dsend[k, d] = combine(0, d)
                pair_copy(k).start()
                for d in range(n_chip):
                    z[k, d] = combine(1, d)

        o[rows // ALIGN:] = jnp.zeros((WIN // ALIGN, ALIGN, CW), BF16)

        @pl.loop(0, (chunks + LAG + 1) // 2)
        def _(k2):
            one_step(k2 * 2, 0)
            one_step(k2 * 2 + 1, 1)

        @pl.loop(0, chunks)
        def _(k):
            pair_copy(k).wait_send()
            for cp in s1_copies(k) + s2_copies(k):
                cp.wait_send()

    pl.run_scoped(give_back, pltpu.VMEM(((rows + WIN) // ALIGN, ALIGN, CW), BF16),
                  pltpu.VMEM((chunks, n_chip, tok, CW), F32), pltpu.VMEM((chunks, n_chip, tok, CW), F32),
                  pltpu.VMEM((chunks, 2, half, CW), F32))


def solution(mesh):
    n_dev = mesh.shape['ep']

    def device_step(tokens, expert_ids, norm_gain, w_router, w_gate, w_up, w_down):
        tok, top_k = expert_ids.shape
        width = tokens.shape[1]
        e_local, _, ff = w_gate.shape
        n_chip = n_dev // 2
        recv_max = 3 * tok * top_k // 2
        nb = (recv_max - e_local) // BR + e_local
        rows = nb * BR
        chunks = width // CW
        dma = pltpu.SemaphoreType.DMA
        half_blk = (chunks, 2, tok // 2, CW)
        tabs = (8 + n_dev * 8, 128)
        wbuf = pltpu.VMEM((e_local, width, 2 * FC), BF16)
        return pl.pallas_call(
            functools.partial(moe_kernel, n_dev, nb, chunks),
            name='moe',
            out_shape=jax.ShapeDtypeStruct((tok, width), BF16),
            in_specs=[VM] * 4 + [ANY] * 3,
            out_specs=VM,
            scratch_shapes=[pltpu.VMEM((n_chip, 2 * tok, width), BF16), wbuf, wbuf,
                            pltpu.VMEM((rows, ff), BF16),
                            pltpu.VMEM((2, n_chip, e_local, tok, WIN), BF16),
                            pltpu.VMEM((2, n_chip, e_local, tok, 128), F32),
                            pltpu.VMEM((n_dev, top_k, tok), I32),
                            pltpu.VMEM((n_dev * 8, tok), F32),
                            pltpu.VMEM(tabs, I32), pltpu.SMEM(tabs, I32),
                            pltpu.VMEM((chunks, n_chip, tok, CW), F32),
                            pltpu.VMEM(half_blk, F32), pltpu.VMEM(half_blk, F32), pltpu.VMEM(half_blk, F32),
                            dma((3, 2)), dma(()), dma((n_dev - 1,)), dma((n_dev,)), dma((14,)), dma((n_dev, 2)),
                            dma((chunks,)), dma((chunks,)),
                            dma((chunks, 4)), dma((chunks, 2)), dma((chunks, 2)), dma((chunks, 2)), dma((chunks, 2))],
            compiler_params=pltpu.CompilerParams(vmem_limit_bytes=67043328, collective_id=0, has_side_effects=True),
        )(tokens, expert_ids.T, norm_gain, w_router.T, w_gate, w_up, w_down)

    row_spec = P(('dp', 'ep'), None)
    expert_spec = P('ep', None, None)
    return jax.shard_map(device_step, mesh=mesh, in_specs=(row_spec, row_spec, P(None), P(None, None), expert_spec, expert_spec, expert_spec), out_specs=row_spec, check_vma=False)
```

```python
import functools

import jax
import jax.numpy as jnp
from jax import lax
from jax.experimental import pallas as pl
from jax.experimental.pallas import tpu as pltpu
from jax.sharding import PartitionSpec as P

NORM_EPS = 1e-5
BR = 128
WIN = 256
ALIGN = 16
FC = 128
CW = 256
LAG = 5
F32 = jnp.float32
BF16 = jnp.bfloat16
I32 = jnp.int32
MESH = pl.DeviceIdType.MESH
ANY = pl.BlockSpec(memory_space=pl.ANY)
VM = pl.BlockSpec(memory_space=pltpu.VMEM)


def moe_kernel(n_dev, nb, chunks, x_hbm, ids_hbm, g_hbm, wr_hbm, w1_hbm, w3_hbm, w2_hbm, o_ref,
               x_ref, ids_ref, g_ref, wr_ref, u, wb0, wb1, h, pt, gb, ids, posm, tab_v, tab, drecv, r1, rd, r2,
               insem, wsem, tsem, ids_ssem, ids_rsem, ssem, rsem,
               d_ss, d_rs, s1_ss, r1_rs, rd_rs, s2_ss, r2_rs):
    n_chip = n_dev // 2
    tok, width = x_ref.shape
    half = tok // 2
    top_k = ids_ref.shape[0]
    e_local, ff = w2_hbm.shape[0], w2_hbm.shape[1]
    rows = nb * BR
    f_steps = ff // FC
    wbs = (wb0, wb1)

    def rcopy(src, dst, ss, rs, peer):
        return pltpu.make_async_remote_copy(src, dst, ss, rs, device_id={'ep': peer}, device_id_type=MESH)

    def expert_of(b):
        return jnp.minimum(jnp.maximum(tab[0, b], 0), e_local - 1)

    def window_of(s, e):
        return jnp.minimum(jnp.maximum(tab[8 + s * 8 + e, 0], 0), rows // ALIGN)

    def coords():
        me = lax.axis_index('ep')
        chip, core = me // 2, me % 2
        rc, lc, oc = (chip + 1) % n_chip, (chip + n_chip - 1) % n_chip, (chip + 2) % n_chip
        return me, chip, core, rc, lc, oc, rc * 2 + core, lc * 2 + core, chip * 2 + (1 - core)

    def hidden_copies(f, i):
        cols = pl.ds(pl.multiple_of(f * FC, FC), FC)
        return (pltpu.make_async_copy(w1_hbm.at[:, :, cols], wbs[i].at[:, :, 0:FC], wsem.at[0, i]),
                pltpu.make_async_copy(w3_hbm.at[:, :, cols], wbs[i].at[:, :, FC:2 * FC], wsem.at[1, i]))

    def down_copy(k, i):
        return pltpu.make_async_copy(w2_hbm.at[:, :, pl.ds(pl.multiple_of(k * CW, CW), CW)],
                                     wbs[i].at[:, 0:ff, :], wsem.at[2, i])

    def dispatch(p, xs):
        me, chip, core, rc, lc, oc, right, left, partner = coords()
        others = [(me + i) % n_dev for i in range(1, n_dev)]
        inputs = [pltpu.make_async_copy(src, dst, insem.at[i]) for i, (src, dst) in enumerate(
            ((x_hbm, x_ref), (g_hbm, g_ref), (ids_hbm, ids_ref), (wr_hbm, wr_ref)))]
        for cp in inputs:
            cp.start()
        barrier = pltpu.get_barrier_semaphore()
        for peer in others:
            pl.semaphore_signal(barrier, inc=1, device_id={'ep': peer}, device_id_type=MESH)

        for cp in inputs:
            cp.wait()
        for i in range(2):
            for cp in hidden_copies(i, i):
                cp.start()

        gain = g_ref[...].astype(F32).reshape(1, width)
        step = tok // 4
        for i in range(4):
            x32 = x_ref[i * step:(i + 1) * step, :].astype(F32)
            inv = lax.rsqrt(jnp.mean(x32 * x32, axis=1, keepdims=True) + NORM_EPS)
            u[chip, pl.ds(pl.multiple_of((i // 2) * tok + core * half + (i % 2) * step, step), step), :] = (x32 * inv * gain).astype(BF16)
        pl.semaphore_wait(barrier, n_dev - 1)

        def send(i, blk, hf, peer):
            ref = u.at[blk // 2, pl.ds(pl.multiple_of(hf * tok + (blk % 2) * half, half), half), :]
            return rcopy(ref, ref, ssem.at[i], rsem.at[blk, hf], peer)

        def ids_send(i, peer):
            return rcopy(ids_ref, ids.at[me], ids_ssem.at[i], ids_rsem.at[me], peer)

        for i, peer in enumerate(others):
            ids_send(i, peer).start()
        sends = [send(0, me, 0, right), send(1, me, 1, left), send(2, me, 0, partner), send(3, me, 1, partner),
                 send(4, me, 1, right), send(5, me, 0, left)]
        for s in sends:
            s.start()

        def arrived(blk, hf):
            send(0, blk, hf, partner).wait_recv()

        def forward(i, blk, hf, peer):
            s = send(i, blk, hf, peer)
            s.start()
            sends.append(s)

        ids[me] = ids_ref[...]
        for i in range(1, n_dev):
            src = (me + i) % n_dev
            rcopy(ids_ref, ids.at[src], ids_ssem.at[0], ids_rsem.at[src], partner).wait_recv()
        sub = lax.broadcasted_iota(I32, (e_local, tok), 0)
        gid = sub + me * e_local
        hits = []
        for s in range(n_dev):
            hit = jnp.zeros((e_local, tok), I32)
            for j in range(top_k):
                hit = hit + (ids[s, j:j + 1, :] == gid).astype(I32)
            hits.append(hit.astype(F32))
        hit_all = jnp.concatenate(hits, axis=0).astype(BF16)
        ri = lax.broadcasted_iota(I32, (tok, tok), 0)
        ci = lax.broadcasted_iota(I32, (tok, tok), 1)
        before = (ri < ci).astype(F32).astype(BF16)
        cnt_all = jnp.dot(hit_all, jnp.ones((tok, tok), BF16), preferred_element_type=F32)
        rank_all = jnp.dot(hit_all, before, preferred_element_type=F32)
        total = jnp.zeros((e_local, tok), F32)
        for s in range(n_dev):
            total = total + cnt_all[s * e_local:(s + 1) * e_local, :]
        blocks = jnp.floor((total + (BR - 1)) * (1.0 / BR))
        first = jnp.zeros((e_local, tok), F32)
        for e in range(e_local - 1):
            first = first + jnp.where(sub > e, jnp.broadcast_to(blocks[e:e + 1, :], (e_local, tok)), 0.0)
        last = first + blocks
        lane = lax.broadcasted_iota(I32, (e_local, tok), 1).astype(F32)
        blk_exp = jnp.sum(jnp.where(lane >= last, 1.0, 0.0), axis=0, keepdims=True)
        tab_v[0:8, :] = jnp.broadcast_to(jnp.minimum(blk_exp, e_local - 1.0), (8, tok)).astype(I32)
        carry = jnp.zeros((e_local, tok), F32)
        starts, rels = [], []
        for s in range(n_dev):
            run = first * BR + carry
            pos = run + rank_all[s * e_local:(s + 1) * e_local, :]
            start = jnp.floor(run * (1.0 / ALIGN))
            tab_v[8 + s * 8:16 + s * 8, :] = jnp.minimum(start, 1.0 * (rows // ALIGN)).astype(I32)
            rels.append(jnp.where(hits[s] > 0, pos - start * ALIGN, -1.0))
            posm[s * 8:(s + 1) * 8, :] = jnp.where(hits[s] > 0, pos + 1.0, 0.0)
            carry = carry + cnt_all[s * e_local:(s + 1) * e_local, :]
        tab_copy = pltpu.make_async_copy(tab_v, tab, tsem)
        tab_copy.start()
        row_i = lax.broadcasted_iota(I32, (BR, tok), 0).astype(F32)

        @pl.loop(0, nb)
        def _(b):
            bf = b.astype(F32)
            mine = (first <= bf) & (bf < last)
            rs = pl.ds(pl.multiple_of(b * BR, BR), BR)
            sel = [jnp.sum(jnp.where(mine, posm[s * 8:(s + 1) * 8, :], 0.0), axis=0, keepdims=True) - (1.0 + BR * bf)
                   for s in range(n_dev)]
            for c in range(n_chip):
                for hf in range(2):
                    cut = slice(hf * half, (hf + 1) * half)
                    both = jnp.concatenate([sel[2 * c][:, cut], sel[2 * c + 1][:, cut]], axis=1)
                    p[c, rs, hf * tok:(hf + 1) * tok] = jnp.where(
                        jnp.broadcast_to(both, (BR, tok)) == row_i, 1.0, 0.0).astype(BF16)

        def windows():
            wlane = lax.broadcasted_iota(I32, (tok, WIN), 1).astype(F32)
            for s in range(n_dev):
                rel_t = jnp.concatenate([rels[s], jnp.zeros((tok - e_local, tok), F32)], axis=0).T
                par = (s % 2 + core + 1) % 2
                for e in range(e_local):
                    col = jnp.broadcast_to(rel_t[:, e:e + 1], (tok, WIN))
                    pt[par, s // 2, e] = jnp.where(col == wlane, 1.0, 0.0).astype(BF16)

        def gates(c):
            logits = lax.dot_general(u[c], wr_ref[...], (((1,), (1,)), ((), ())), preferred_element_type=F32)
            ex = jnp.exp(logits - jnp.max(logits, axis=1, keepdims=True))
            prob = ex / jnp.sum(ex, axis=1, keepdims=True)
            full = jnp.concatenate([prob, jnp.zeros((2 * tok, 128 - prob.shape[1]), F32)], axis=1)
            mine = pltpu.roll(full, (128 - me * e_local) % 128, 1)
            for k in range(2):
                par = (k + core + 1) % 2
                own = jnp.concatenate([mine[k * half:(k + 1) * half], mine[tok + k * half:tok + (k + 1) * half]], axis=0)
                for e in range(e_local):
                    gb[par, c, e] = jnp.broadcast_to(own[:, e:e + 1], (tok, 128))

        mt, nt = rows // 4, 256

        def gather(pieces, first_pass):
            @pl.loop(0, rows // mt)
            def _(m):
                rs = pl.ds(pl.multiple_of(m * mt, mt), mt)
                pick = [p[c, rs, a:b] for c, a, b in pieces]
                pick = pick[0] if len(pick) == 1 else jnp.concatenate(pick, axis=1)
                for n in range(width // nt):
                    cols = slice(n * nt, (n + 1) * nt)
                    tile = [u[c, a:b, cols] for c, a, b in pieces]
                    tile = tile[0] if len(tile) == 1 else jnp.concatenate(tile, axis=0)
                    part = jnp.dot(pick, tile, preferred_element_type=F32).astype(BF16)
                    if first_pass:
                        xs[rs, cols] = part
                    else:
                        xs[rs, cols] = xs[rs, cols] + part

        l_other, r_other, o_own, o_other = lc * 2 + (1 - core), rc * 2 + (1 - core), oc * 2 + core, oc * 2 + (1 - core)
        arrived(partner, 0)
        arrived(partner, 1)
        gather([(chip, 0, 2 * tok)], True)
        arrived(left, 0)
        forward(6, left, 0, right)
        arrived(right, 1)
        forward(7, right, 1, left)
        forward(8, left, 0, partner)
        forward(9, right, 1, partner)
        windows()
        gates(chip)
        arrived(l_other, 0)
        arrived(r_other, 1)
        gather([(lc, 0, tok), (rc, tok, 2 * tok)], False)
        arrived(left, 1)
        forward(10, left, 1, partner)
        arrived(right, 0)
        forward(11, right, 0, partner)
        arrived(l_other, 1)
        arrived(r_other, 0)
        gather([(lc, tok, 2 * tok), (rc, 0, tok)], False)
        arrived(o_own, 0)
        forward(12, o_own, 0, partner)
        arrived(o_own, 1)
        forward(13, o_own, 1, partner)
        gates(lc)
        gates(rc)
        arrived(o_other, 0)
        arrived(o_other, 1)
        gather([(oc, 0, 2 * tok)], False)
        gates(oc)
        tab_copy.wait()

        @pl.loop(0, f_steps // 2)
        def _(f2):
            for i in range(2):
                f = f2 * 2 + i
                for cp in hidden_copies(f, i):
                    cp.wait()
                for b in range(nb):
                    r = jnp.dot(xs[b * BR:(b + 1) * BR, :], wbs[i][expert_of(b)], preferred_element_type=F32)
                    hg, hu = r[:, 0:FC], r[:, FC:2 * FC]
                    h[b * BR:(b + 1) * BR, pl.ds(pl.multiple_of(f * FC, FC), FC)] = (hg * jax.nn.sigmoid(hg) * hu).astype(BF16)

                @pl.when(f + 2 < f_steps)
                def _():
                    for cp in hidden_copies(f + 2, i):
                        cp.start()

                @pl.when(f + 2 >= f_steps)
                def _():
                    down_copy(i, i).start()

        for s in sends:
            s.wait_send()
        for i, peer in enumerate(others):
            ids_send(i, peer).wait_send()

    pl.run_scoped(dispatch, pltpu.VMEM((n_chip, rows, 2 * tok), BF16), pltpu.VMEM((rows, width), BF16))

    lo, hi = pl.ds(0, half), pl.ds(half, half)

    def give_back(o, dsend, z, s2):
        _, chip, core, rc, lc, oc, right, left, partner = coords()

        def pair_copy(k):
            return rcopy(dsend.at[k], drecv.at[k], d_ss.at[k], d_rs.at[k], partner)

        def s1_copies(k):
            return (rcopy(z.at[k, oc, lo, :], r1.at[k, 0], s1_ss.at[k, 0], r1_rs.at[k, 0], right),
                    rcopy(z.at[k, oc, hi, :], r1.at[k, 1], s1_ss.at[k, 1], r1_rs.at[k, 1], left),
                    rcopy(z.at[k, lc, lo, :], rd.at[k, 0], s1_ss.at[k, 2], rd_rs.at[k, 0], left),
                    rcopy(z.at[k, rc, hi, :], rd.at[k, 1], s1_ss.at[k, 3], rd_rs.at[k, 1], right))

        def s2_copies(k):
            return (rcopy(s2.at[k, 0], r2.at[k, 0], s2_ss.at[k, 0], r2_rs.at[k, 0], right),
                    rcopy(s2.at[k, 1], r2.at[k, 1], s2_ss.at[k, 1], r2_rs.at[k, 1], left))

        def combine(par, d):
            s = d * 2 + (core if par == 1 else 1 - core)
            acc = jnp.zeros((tok, CW), F32)
            for e in range(e_local):
                win = o[pl.ds(window_of(s, e), WIN // ALIGN)].reshape(WIN, CW)
                m = jnp.dot(pt[par, d, e], win, preferred_element_type=F32)
                acc = acc + jnp.concatenate([gb[par, d, e]] * (CW // 128), axis=1) * m
            return acc

        def one_step(k, i):
            @pl.when((k >= 5) & (k < chunks + 5))
            def _():
                kk = k - 5
                r2c, s1c = s2_copies(kk), s1_copies(kk)
                cols = pl.ds(pl.multiple_of(kk * CW, CW), CW)
                for j, rs in enumerate((lo, hi)):
                    r2c[j].wait_recv()
                    s1c[2 + j].wait_recv()
                    tot = z[kk, chip, rs, :] + r2[kk, j] + rd[kk, j] + x_ref[rs, cols].astype(F32)
                    o_ref[rs, cols] = tot.astype(BF16)

            @pl.when((k >= 3) & (k < chunks + 3))
            def _():
                kk = k - 3
                s1c, s2c = s1_copies(kk), s2_copies(kk)
                s1c[0].wait_recv()
                s2[kk, 0] = r1[kk, 0] + z[kk, rc, lo, :]
                s2c[0].start()
                s1c[1].wait_recv()
                s2[kk, 1] = r1[kk, 1] + z[kk, lc, hi, :]
                s2c[1].start()

            @pl.when(k < chunks)
            def _():
                down_copy(k, i).wait()
                for b in range(nb):
                    ob = jnp.dot(h[b * BR:(b + 1) * BR, :], wbs[i][expert_of(b), 0:ff, :], preferred_element_type=F32)
                    o[b * BR // ALIGN:(b + 1) * BR // ALIGN] = ob.astype(BF16).reshape(BR // ALIGN, ALIGN, CW)

            @pl.when(k + 2 < chunks)
            def _():
                down_copy(k + 2, i).start()

            @pl.when((k >= 1) & (k < chunks + 1))
            def _():
                kk = k - 1
                pair_copy(kk).wait_recv()
                for d in range(n_chip):
                    z[kk, d] = z[kk, d] + drecv[kk, d]
                for cp in s1_copies(kk):
                    cp.start()

            @pl.when(k < chunks)
            def _():
                for d in range(n_chip):
                    dsend[k, d] = combine(0, d)
                pair_copy(k).start()
                for d in range(n_chip):
                    z[k, d] = combine(1, d)

        o[rows // ALIGN:] = jnp.zeros((WIN // ALIGN, ALIGN, CW), BF16)

        @pl.loop(0, (chunks + LAG + 1) // 2)
        def _(k2):
            one_step(k2 * 2, 0)
            one_step(k2 * 2 + 1, 1)

        @pl.loop(0, chunks)
        def _(k):
            pair_copy(k).wait_send()
            for cp in s1_copies(k) + s2_copies(k):
                cp.wait_send()

    pl.run_scoped(give_back, pltpu.VMEM(((rows + WIN) // ALIGN, ALIGN, CW), BF16),
                  pltpu.VMEM((chunks, n_chip, tok, CW), F32), pltpu.VMEM((chunks, n_chip, tok, CW), F32),
                  pltpu.VMEM((chunks, 2, half, CW), F32))


def solution(mesh):
    n_dev = mesh.shape['ep']

    def device_step(tokens, expert_ids, norm_gain, w_router, w_gate, w_up, w_down):
        tok, top_k = expert_ids.shape
        width = tokens.shape[1]
        e_local, _, ff = w_gate.shape
        n_chip = n_dev // 2
        recv_max = 3 * tok * top_k // 2
        nb = (recv_max - e_local) // BR + e_local
        rows = nb * BR
        chunks = width // CW
        dma = pltpu.SemaphoreType.DMA
        half_blk = (chunks, 2, tok // 2, CW)
        tabs = (8 + n_dev * 8, 128)
        wbuf = pltpu.VMEM((e_local, width, 2 * FC), BF16)
        return pl.pallas_call(
            functools.partial(moe_kernel, n_dev, nb, chunks),
            name='moe',
            out_shape=jax.ShapeDtypeStruct((tok, width), BF16),
            in_specs=[ANY] * 7,
            out_specs=VM,
            scratch_shapes=[pltpu.VMEM((tok, width), BF16), pltpu.VMEM((top_k, tok), I32), pltpu.VMEM((width,), BF16),
                            pltpu.VMEM((w_router.shape[1], width), BF16),
                            pltpu.VMEM((n_chip, 2 * tok, width), BF16), wbuf, wbuf,
                            pltpu.VMEM((rows, ff), BF16),
                            pltpu.VMEM((2, n_chip, e_local, tok, WIN), BF16),
                            pltpu.VMEM((2, n_chip, e_local, tok, 128), F32),
                            pltpu.VMEM((n_dev, top_k, tok), I32),
                            pltpu.VMEM((n_dev * 8, tok), F32),
                            pltpu.VMEM(tabs, I32), pltpu.SMEM(tabs, I32),
                            pltpu.VMEM((chunks, n_chip, tok, CW), F32),
                            pltpu.VMEM(half_blk, F32), pltpu.VMEM(half_blk, F32), pltpu.VMEM(half_blk, F32),
                            dma((4,)), dma((3, 2)), dma(()), dma((n_dev - 1,)), dma((n_dev,)), dma((14,)), dma((n_dev, 2)),
                            dma((chunks,)), dma((chunks,)),
                            dma((chunks, 4)), dma((chunks, 2)), dma((chunks, 2)), dma((chunks, 2)), dma((chunks, 2))],
            compiler_params=pltpu.CompilerParams(vmem_limit_bytes=67043328, collective_id=0, has_side_effects=True),
        )(tokens, expert_ids.T, norm_gain, w_router.T, w_gate, w_up, w_down)

    row_spec = P(('dp', 'ep'), None)
    expert_spec = P('ep', None, None)
    return jax.shard_map(device_step, mesh=mesh, in_specs=(row_spec, row_spec, P(None), P(None, None), expert_spec, expert_spec, expert_spec), out_specs=row_spec, check_vma=False)
```
